32 devices in a mesh: level: 2 (over core), group: 8 (over z, y), leaf: 2 (over x).
Axes of the slice: x: 2, y: 2, z: 4, core: 2. Of those that a mesh axis runs over, the one named last changes fastest.
Arguments:
- queries: bfloat16 [768, 2048], P('group'), may hold values from -6 to 6
- weights: bfloat16 [2, 2, 8, 2048, 1024], P('level', 'leaf', 'group'), may hold values from -0.125 to 0.125
- block_mask: int32 [2, 2, 8, 16], P('level', 'leaf', 'group'), may hold values 0 or 1
- label_map: int32 [2, 2, 8, 1024], P('level', 'leaf', 'group'), may hold values from 0 to 1023, each once within a row
- beam_lists: int32 [2, 768, 4], P('level', 'group'), may hold values from 0 to 7, all different within a row; in each aligned block of 32 rows (0 to 31, 32 to 63, ..., all dimensions but the last counted through in order) at most 32 rows name the same one
- root_score: bfloat16 [768, 4], P('group'), may hold values from 0.19921875 to 1
- parent_pos: int32 [768, 4], P('group'), may hold values from 0 to 4095
Outputs:
- scores: float32 [2, 768, 4, 1024], P('level', 'group', None, 'leaf')
The draws below stay inside these ranges and needn't reach their ends.
Inputs may be any that keep to these rules, and one draw needn't show every extreme that they name: `beam_lists`: each row names 4 different groups; in each aligned block of 32 rows (both levels' rows taken in order) no group is named by more than 32 rows, a bound that some block reaches. `label_map`: each row is a permutation of 0 to 1023.
All inputs are finite; a program needn't handle non-finite values. No bound on the sum of `block_mask` on one device may be relied on, other than what follows from the above.
Results may differ from the reference program's by a relative error of at most 0.0013.
Values may be sent and summed in bfloat16 or wider, within the bound.
No kernel may reach another device: no remote copies, remote signals or barrier semaphores. Data moves between devices by JAX's collectives and lax.ppermute only.
A program may use at most 128 MiB of HBM per device.

```python
import math
import jax
import jax.numpy as jnp
import numpy as np
from jax import lax

D = 2048
L = 1024
B = 4
QBLK = 32
MASKB = 16
GROUPS = 8
CAP = 32
TREES = 2
QUERIES = 768


def touch_ends(array, key, least, largest):
    extent = array.shape
    index_at = [jax.random.randint(jax.random.fold_in(key, axis), (), 0, extent[axis]) for axis in range(len(extent))]
    array = array.at[tuple(index_at)].set(least)
    longest = extent.index(max(extent))
    index_at[longest] = (index_at[longest] + 1) % extent[longest]
    return array.at[tuple(index_at)].set(largest)


def block_levels(own_key, extent, shards, low, largest):
    level = 1.0
    for position, parts in shards:
        steps = jax.random.uniform(jax.random.fold_in(jax.random.fold_in(own_key, 6), position), (parts,), jnp.float32, low / len(shards), largest / len(shards))
        level = level * jnp.repeat(jnp.exp(steps), extent[position] // parts).reshape((-1,) + (1,) * (len(extent) - 1 - position))
    return level


def shared_out(own_key, own, number, rows, number_of, top, limit, lean):
    order = jax.random.permutation(own_key, number_of)
    heavy_load, usual = shares(number_of, rows * top, limit, lean, True), shares(number_of, rows * top, limit, lean, False)
    places = jnp.arange(number_of)

    def named(lengths, rotation):
        used = int((lengths > 0).sum())
        fixed = max(1, used // 4)
        moved = fixed + (places - fixed + rotation * (used - fixed)) % max(1, number_of - fixed)
        return jnp.zeros((number_of,), jnp.int32).at[order[jnp.where(places < fixed, places, moved)]].set(jnp.asarray(lengths, jnp.int32))

    lengths = jnp.where(number % 4 == 0, named(heavy_load, number // 4), named(usual, number - number // 4 - 1))
    mixed = jax.random.permutation(jax.random.fold_in(own, 3), number_of)
    giver, receiver = mixed[0:number_of // 2 * 2:2], mixed[1:number_of // 2 * 2:2]
    margin = jnp.minimum(lengths[giver] - 1, limit - lengths[receiver]) // 2
    margin = jnp.where((giver == order[0]) | (receiver == order[0]) | (lengths[receiver] == 0), 0, jnp.maximum(margin, 0))
    moved = jax.random.randint(jax.random.fold_in(own, 4), (number_of // 2,), 0, 1 << 20) % (margin + 1)
    lengths = lengths.at[giver].add(-moved).at[receiver].add(moved)
    labels = jnp.searchsorted(jnp.cumsum(lengths), jnp.arange(rows * top), side="right").astype(jnp.int32)
    table = labels.reshape(top, rows).T
    table = table[jax.random.permutation(jax.random.fold_in(own, 1), rows)]
    rotation = jax.random.randint(jax.random.fold_in(own, 2), (rows, 1), 0, top)
    return jnp.take_along_axis(table, (jnp.arange(top)[None, :] + rotation) % top, axis=1)


def shares(number_of, total, bound, slope, full):
    portions = [(1 << 20) // math.isqrt(grade ** slope) + 1 for grade in range(1, number_of + 1)]
    largest = bound if full else min(bound, max(-(-total // number_of), total * portions[0] // sum(portions)))
    least = 1 if total - largest >= number_of - 1 else 0
    holding, spare = [largest] + [least] * (number_of - 1), total - largest - least * (number_of - 1)
    while spare > 0:
        movable = [i for i in range(1, number_of) if holding[i] < largest] or [i for i in range(1, number_of) if holding[i] < bound]
        pool, remaining = sum([portions[i] for i in movable]), spare
        for i in movable:
            extra = min(bound - holding[i], max(1, remaining * portions[i] // pool), spare)
            holding[i] = holding[i] + extra
            spare = spare - extra
    return np.array(holding)


def centred(own_key, shape, scale, reach, split=(), held_as=jnp.bfloat16):
    factor_of = block_levels(own_key, shape, split, -0.22, 0.18) if split else 1.0
    values = jax.random.normal(own_key, shape, jnp.float32) * scale * factor_of
    return jnp.minimum(jnp.maximum(values, -reach), reach).astype(held_as)


def setup_inputs(seed: int = 0) -> dict:
    seeds = jax.random.split(jax.random.key(seed), 8)
    queries = centred(seeds[0], (QUERIES, D), 1.0, 6.0, ((0, 8),))
    weights = centred(seeds[1], (2, TREES, GROUPS, D, L), D ** -0.5, 0.125, ((0, 2), (1, 2), (2, 8)))
    block_mask = touch_ends((jax.random.randint(seeds[2], (2, TREES, GROUPS, MASKB), 0, 4) < 3).astype(jnp.int32), jax.random.fold_in(seeds[2], 1), 0, 1)
    label_map = jax.vmap(lambda own: jax.random.permutation(own, L))(jax.random.split(seeds[3], 2 * TREES * GROUPS)).reshape((2, TREES, GROUPS, L)).astype(jnp.int32)
    beam_lists_keys = jax.random.split(jax.random.fold_in(seeds[4], 1), 2 * QUERIES // QBLK)
    beam_lists_turns = jax.random.permutation(jax.random.fold_in(seeds[4], 3), 2 * QUERIES // QBLK)
    beam_lists = jax.vmap(lambda own, number: shared_out(jax.random.fold_in(seeds[4], 2), own, number, QBLK, GROUPS, B, CAP, 2))(beam_lists_keys, beam_lists_turns).reshape((2, QUERIES, B))
    root_score = jnp.clip(0.19921875 + 0.80078125 * jax.random.uniform(seeds[5], (QUERIES, B), jnp.float32) ** block_levels(seeds[5], (QUERIES, B), ((0, 8),), -0.2, 0.2), 0.19921875, 1.0).astype(jnp.bfloat16)
    parent_pos = touch_ends(jax.random.randint(seeds[6], (QUERIES, B), 0, B * L), jax.random.fold_in(seeds[6], 1), 0, (B * L) - 1).astype(jnp.int32)
    return dict(queries=queries, weights=weights, block_mask=block_mask, label_map=label_map, beam_lists=beam_lists, root_score=root_score, parent_pos=parent_pos)


def tree_level(queries, scorer, keep_mask, label_map, beam_list, parent):
    groups = scorer.shape[0]
    feature = scorer.shape[1]
    label_width = scorer.shape[2]
    beam_len = beam_list.shape[1]
    flat_beam = beam_list.reshape(-1)
    flat_parent = parent.reshape(-1).astype(jnp.float32)
    most_rows = (QUERIES // QBLK) * CAP

    def visit_group(summed, group_id):
        hitting = flat_beam == group_id
        entries = jnp.nonzero(hitting, size=most_rows, fill_value=0)[0].astype(jnp.int32)
        active = jnp.arange(most_rows, dtype=jnp.int32) < jnp.sum(hitting.astype(jnp.int32))
        routed = queries[entries // beam_len]
        keeping = jnp.repeat(keep_mask[group_id], feature // keep_mask.shape[1]).astype(scorer.dtype)
        masked = scorer[group_id] * keeping[:, None]
        logits = jnp.dot(routed, masked, preferred_element_type=jnp.float32)
        scored = jax.nn.sigmoid(logits) * flat_parent[entries][:, None]
        scored = scored[:, label_map[group_id]]
        scored = jnp.where(active[:, None], scored, jnp.zeros_like(scored))
        return summed.at[entries].add(scored), None

    initial = jnp.zeros((flat_beam.shape[0], label_width), jnp.float32)
    summed, _ = lax.scan(visit_group, initial, jnp.arange(groups, dtype=jnp.int32))
    return summed.reshape(beam_list.shape[0], beam_len, label_width)


def reference(queries, weights, block_mask, label_map, beam_lists, root_score, parent_pos):
    first_level = jnp.zeros((QUERIES, B, L), jnp.float32)
    for member in range(TREES):
        first_level = first_level + tree_level(queries, weights[0, member], block_mask[0, member], label_map[0, member], beam_lists[0], root_score)
    picked = jnp.take_along_axis(first_level.reshape(QUERIES, B * L), parent_pos, axis=1) / TREES
    second_parent = picked.astype(jnp.bfloat16)
    second = jnp.zeros((QUERIES, B, L), jnp.float32)
    for member in range(TREES):
        second = second + tree_level(queries, weights[1, member], block_mask[1, member], label_map[1, member], beam_lists[1], second_parent)
    return jnp.stack([first_level, second])
```

```python
import functools

import jax
import jax.numpy as jnp
from jax import lax
from jax.experimental import pallas as pl
from jax.experimental.pallas import tpu as pltpu
from jax.sharding import PartitionSpec as P

LANES = 128
TAIL = 16
STEPS = 65535.0
LEAST = 1e-30
VMEM = pl.BlockSpec(memory_space=pltpu.VMEM)
SMEM = pl.BlockSpec(memory_space=pltpu.SMEM)


def swapped(block, axis, distance):
    devices = range(lax.axis_size(axis))
    return lax.ppermute(block, axis, [(i, i ^ distance) for i in devices])


def params():
    return pltpu.CompilerParams(vmem_limit_bytes=60 * 1024 * 1024)


def lane_iota(shape, axis):
    return lax.broadcasted_iota(jnp.int32, shape, axis)


def nt_dot(a, b):
    return lax.dot_general(a, b, (((1,), (1,)), ((), ())), preferred_element_type=jnp.float32)


def encode(scores):
    top = jnp.max(scores, axis=1, keepdims=True)
    power = jnp.ceil(jnp.log2(jnp.maximum(top, LEAST)))
    units = jnp.minimum(jnp.round(scores * (jnp.exp2(-power) * STEPS)), STEPS)
    return (units.astype(jnp.int32) - 32768).astype(jnp.int16), power


def tail_of(powers):
    total = jnp.zeros((TAIL, LANES), jnp.float32)
    for i, power in enumerate(powers):
        rows = power.shape[0]
        wide = jnp.broadcast_to(power, (rows, LANES)).astype(jnp.bfloat16)
        if rows < LANES:
            wide = jnp.concatenate([wide, jnp.zeros((LANES - rows, LANES), jnp.bfloat16)], axis=0)
        shape = (TAIL, LANES)
        pick = (lane_iota(shape, 0) == i) & (lane_iota(shape, 1) == 0)
        total = total + nt_dot(pick.astype(jnp.bfloat16), wide)
    return total.astype(jnp.int32).astype(jnp.int16)


def scale_of(tail, i, rows):
    held = tail.astype(jnp.int32).astype(jnp.float32)[i : i + 1, :]
    spread = jnp.broadcast_to(held, (LANES, LANES)).astype(jnp.bfloat16)
    shape = (LANES, LANES)
    unit = (lane_iota(shape, 0) == lane_iota(shape, 1)).astype(jnp.bfloat16)
    return (jnp.exp2(nt_dot(unit, spread)) * (1.0 / STEPS))[:rows]


def units_of(codes):
    return codes.astype(jnp.int32).astype(jnp.float32) + 32768.0


def prepare_kernel(leaf_count, mask_rows, mask_ref, label_ref, weight_ref, out_ref, onehot_ref):
    step = pl.program_id(0)
    rows, width = weight_ref.shape
    share = width // leaf_count

    @pl.when(step == 0)
    def _():
        leaf = lax.axis_index("leaf")
        for d in range(leaf_count):
            wanted = label_ref[pl.ds(jnp.bitwise_xor(leaf, d), 1), :]
            column = lane_iota((width, share), 0)
            onehot_ref[:, d * share : (d + 1) * share] = (column == wanted).astype(jnp.bfloat16)

    per = rows // mask_rows
    kept = []
    for i in range(per):
        part = weight_ref[i * mask_rows : (i + 1) * mask_rows, :]
        keep = mask_ref[0, step * per + i].astype(jnp.float32).astype(jnp.bfloat16)
        kept.append(part * keep)
    kept = jnp.concatenate(kept, axis=0)
    out_ref[...] = jnp.dot(
        kept, onehot_ref[...], preferred_element_type=jnp.float32
    ).astype(jnp.bfloat16)


def prepare(scorer, mask, labels, leaf_count):
    feature, width = scorer.shape
    mask_rows = feature // mask.shape[1]
    tile = min(feature, 4 * mask_rows)
    return pl.pallas_call(
        functools.partial(prepare_kernel, leaf_count, mask_rows),
        grid=(feature // tile,),
        in_specs=[
            SMEM,
            pl.BlockSpec((leaf_count, width // leaf_count), lambda i: (0, 0)),
            pl.BlockSpec((tile, width), lambda i: (i, 0)),
        ],
        out_specs=pl.BlockSpec((tile, width), lambda i: (i, 0)),
        out_shape=jax.ShapeDtypeStruct((feature, width), jnp.bfloat16),
        scratch_shapes=[pltpu.VMEM((width, width), jnp.bfloat16)],
        compiler_params=params(),
        cost_estimate=pl.CostEstimate(
            flops=2 * feature * width * width, bytes_accessed=4 * feature * width, transcendentals=0
        ),
        name="prepare",
    )(mask, labels, scorer)


def score_kernel(blocks, leaf_count, *refs):
    mine_refs, other_refs = refs[:blocks], refs[blocks : 2 * blocks]
    weight_ref = refs[2 * blocks]
    own_ref = refs[2 * blocks + 1]
    sent_refs = refs[2 * blocks + 2 :]
    level = lax.axis_index("level")
    levels = lax.axis_size("level")
    rows, half = mine_refs[0].shape
    share = own_ref.shape[1]
    mine = jnp.concatenate([ref[...] for ref in mine_refs], axis=0)
    other = jnp.concatenate([ref[...] for ref in other_refs], axis=0)
    near = pl.ds(pl.multiple_of(level * half, half), half)
    far = pl.ds(pl.multiple_of((levels - 1 - level) * half, half), half)
    for d in range(leaf_count):
        columns = slice(d * share, (d + 1) * share)
        logits = jnp.dot(mine, weight_ref[near, columns], preferred_element_type=jnp.float32)
        logits = logits + jnp.dot(
            other, weight_ref[far, columns], preferred_element_type=jnp.float32
        )
        scores = jax.nn.sigmoid(logits)
        if d == 0:
            own_ref[...] = scores
        else:
            codes, power = encode(scores)
            out = sent_refs[d - 1]
            out[: blocks * rows, :] = codes
            out[blocks * rows :, :] = jnp.zeros((TAIL, share), jnp.int16)
            out[blocks * rows :, :LANES] = tail_of(
                [power[i * rows : (i + 1) * rows] for i in range(blocks)]
            )


def score(mine, other, weights, leaf_count):
    blocks = len(mine)
    rows = mine[0].shape[0]
    feature, width = weights.shape
    share = width // leaf_count
    message = jax.ShapeDtypeStruct((blocks * rows + TAIL, share), jnp.int16)
    outs = [jax.ShapeDtypeStruct((blocks * rows, share), jnp.float32)] + [message] * (leaf_count - 1)
    return pl.pallas_call(
        functools.partial(score_kernel, blocks, leaf_count),
        in_specs=[VMEM] * (2 * blocks + 1),
        out_specs=[VMEM] * leaf_count,
        out_shape=outs,
        compiler_params=params(),
        cost_estimate=pl.CostEstimate(
            flops=2 * blocks * rows * feature * width,
            bytes_accessed=2 * feature * width,
            transcendentals=2 * blocks * rows * width,
        ),
        name="score",
    )(*mine, *other, weights)


def join_kernel(blocks, rows, *refs):
    own_ref = refs[0]
    got_refs = refs[1 : len(refs) - blocks]
    out_refs = refs[len(refs) - blocks :]
    share = own_ref.shape[1]
    powers = []
    for i in range(blocks):
        span = slice(i * rows, (i + 1) * rows)
        total = own_ref[span, :]
        for ref in got_refs:
            scale = scale_of(ref[blocks * rows :, :LANES], i, rows)
            scale = jnp.concatenate([scale] * (share // LANES), axis=1)
            total = total + units_of(ref[span, :]) * scale
        codes, power = encode(total)
        out_refs[i][:rows, :] = codes
        powers.append(power)
    tail = tail_of(powers)
    for ref in out_refs:
        ref[rows:, :] = jnp.zeros((TAIL, share), jnp.int16)
        ref[rows:, :LANES] = tail


def join(own, got, blocks):
    rows = own.shape[0] // blocks
    share = own.shape[1]
    message = jax.ShapeDtypeStruct((rows + TAIL, share), jnp.int16)
    return pl.pallas_call(
        functools.partial(join_kernel, blocks, rows),
        in_specs=[VMEM] * (1 + len(got)),
        out_specs=[VMEM] * blocks,
        out_shape=[message] * blocks,
        compiler_params=params(),
        cost_estimate=pl.CostEstimate(
            flops=40 * own.size, bytes_accessed=8 * own.size, transcendentals=0
        ),
        name="join",
    )(own, *got)


def gains_of(order, refs, beam, rows, parent):
    me = lax.axis_index("group")
    beam_len = beam.shape[1]
    gains = []
    for (i, k), ref in zip(order, refs):
        scale = scale_of(ref[rows:, :LANES], i, rows)
        owner = jnp.bitwise_xor(me, k)
        row = []
        for b in range(beam_len):
            gain = jnp.where(beam[:, b : b + 1] == owner, scale, 0.0)
            row.append(gain if parent is None else gain * parent[:, b : b + 1])
        gains.append(row)
    return gains


def slab_of(refs, gains, b, rows, lanes):
    total = None
    for ref, row in zip(refs, gains):
        term = units_of(ref[:rows, lanes]) * row[b]
        total = term if total is None else total + term
    return total


def pick_kernel(order, *refs):
    n = len(order)
    got = refs[:n]
    beam_ref, root_ref, parent_ref, out_ref = refs[n:]
    rows, beam_len = beam_ref.shape
    share = got[0].shape[1]
    width = share * lax.axis_size("leaf")
    beam = beam_ref[...]
    gains = gains_of(order, got, beam, rows, root_ref[...].astype(jnp.float32))
    place = parent_ref[...]
    label = place % width - lax.axis_index("leaf") * share
    inside = (label >= 0) & (label < share)
    target = jnp.where(inside, (place // width) * share + label, -1)
    picked = [jnp.zeros((rows, LANES), jnp.float32) for _ in range(beam_len)]
    for b in range(beam_len):
        for start in range(0, share, LANES):
            values = slab_of(got, gains, b, rows, slice(start, start + LANES))
            here = lane_iota((rows, LANES), 1) + (b * share + start)
            for c in range(beam_len):
                picked[c] = picked[c] + jnp.where(here == target[:, c : c + 1], values, 0.0)
    lane = lane_iota((rows, LANES), 1)
    out = jnp.zeros((rows, LANES), jnp.float32)
    for c in range(beam_len):
        out = jnp.where(lane == c, jnp.sum(picked[c], axis=1, keepdims=True), out)
    out_ref[...] = out


def finish_kernel(order, leaf_count, *refs):
    n = len(order)
    got = refs[:n]
    beam_ref, root_ref = refs[n : n + 2]
    picked_refs = refs[n + 2 : n + 2 + leaf_count]
    out_ref = refs[n + 2 + leaf_count]
    rows, beam_len = beam_ref.shape
    share = got[0].shape[1]
    second = picked_refs[0][...]
    for ref in picked_refs[1:]:
        second = second + ref[...]
    second = (second * (1.0 / leaf_count)).astype(jnp.bfloat16).astype(jnp.float32)[:, :beam_len]
    root = root_ref[...].astype(jnp.float32)
    parent = jnp.where(lax.axis_index("level") == 0, root, second)
    gains = gains_of(order, got, beam_ref[...], rows, parent)
    for b in range(beam_len):
        for start in range(0, share, LANES):
            lanes = slice(start, start + LANES)
            out_ref[:, b, lanes] = slab_of(got, gains, b, rows, lanes)


def body(queries, weights, block_mask, label_map, beam_lists, root_score, parent_pos):
    group_count = lax.axis_size("group")
    leaf_count = lax.axis_size("leaf")
    level_count = lax.axis_size("level")
    level = lax.axis_index("level")
    feature, label_width = weights.shape[3:]
    rows = queries.shape[0]
    beam_len = beam_lists.shape[2]
    share = label_width // leaf_count
    half = feature // level_count

    labels = label_map.reshape(leaf_count, share)
    ordered = prepare(weights[0, 0, 0], block_mask.reshape(1, -1), labels, leaf_count)

    mine = {0: lax.dynamic_slice_in_dim(queries, level * half, half, 1)}
    other = {0: lax.dynamic_slice_in_dim(queries, (level_count - 1 - level) * half, half, 1)}
    chunks = [list(range(0, group_count, 2)), list(range(1, group_count, 2))]
    for chunk in chunks:
        for k in chunk:
            if k:
                low = k & -k
                mine[k] = swapped(mine[k ^ low], "group", low)
    for chunk in chunks:
        far = [k for k in chunk if k]
        joined = jnp.concatenate([mine[k] for k in far], axis=0)
        crossed = swapped(joined, "level", 1)
        for i, k in enumerate(far):
            other[k] = crossed[i * rows : (i + 1) * rows]

    messages = {}
    order = []
    for chunk in chunks:
        own, *sent = score([mine[k] for k in chunk], [other[k] for k in chunk], ordered, leaf_count)
        got = [swapped(message, "leaf", d + 1) for d, message in enumerate(sent)]
        for i, (k, message) in enumerate(zip(chunk, join(own, got, len(chunk)))):
            messages[k] = swapped(message, "group", k) if k else message
            order.append((i, k))
    order = tuple(order)
    got = [messages[k] for _, k in order]
    beam = beam_lists[0]

    picked = pl.pallas_call(
        functools.partial(pick_kernel, order),
        in_specs=[VMEM] * (len(got) + 3),
        out_specs=VMEM,
        out_shape=jax.ShapeDtypeStruct((rows, LANES), jnp.float32),
        compiler_params=params(),
        name="pick",
    )(*got, beam, root_score, parent_pos)
    handed = []
    for d in range(leaf_count):
        route = [(leaf, leaf_count + (leaf ^ d)) for leaf in range(leaf_count)]
        handed.append(lax.ppermute(picked, ("level", "leaf"), route))
    scores = pl.pallas_call(
        functools.partial(finish_kernel, order, leaf_count),
        in_specs=[VMEM] * (len(got) + 2 + leaf_count),
        out_specs=VMEM,
        out_shape=jax.ShapeDtypeStruct((rows, beam_len, share), jnp.float32),
        compiler_params=params(),
        name="finish",
    )(*got, beam, root_score, *handed)
    return scores[None]


def solution(mesh):
    in_specs = (
        P("group", None),
        P("level", "leaf", "group", None, None),
        P("level", "leaf", "group", None),
        P("level", "leaf", "group", None),
        P("level", "group", None),
        P("group", None),
        P("group", None),
    )
    out_specs = P("level", "group", None, "leaf")
    return jax.shard_map(body, mesh=mesh, in_specs=in_specs, out_specs=out_specs, check_vma=False)
```

```python
import functools

import jax
import jax.numpy as jnp
from jax import lax
from jax.experimental import pallas as pl
from jax.experimental.pallas import tpu as pltpu
from jax.sharding import PartitionSpec as P

LANES = 128
TAIL = 16
GRANT = 24 * 1024 * 1024
STEPS = 65535.0
LEAST = 1e-30
VMEM = pl.BlockSpec(memory_space=pltpu.VMEM)
SMEM = pl.BlockSpec(memory_space=pltpu.SMEM)


def swapped(block, axis, distance):
    devices = range(lax.axis_size(axis))
    return lax.ppermute(block, axis, [(i, i ^ distance) for i in devices])


def params():
    return pltpu.CompilerParams(vmem_limit_bytes=GRANT)


def lane_iota(shape, axis):
    return lax.broadcasted_iota(jnp.int32, shape, axis)


def nt_dot(a, b):
    return lax.dot_general(a, b, (((1,), (1,)), ((), ())), preferred_element_type=jnp.float32)


def encode(scores):
    top = jnp.max(scores, axis=1, keepdims=True)
    power = jnp.ceil(jnp.log2(jnp.maximum(top, LEAST)))
    units = jnp.minimum(jnp.round(scores * (jnp.exp2(-power) * STEPS)), STEPS)
    return (units.astype(jnp.int32) - 32768).astype(jnp.int16), power


def tail_of(powers):
    total = jnp.zeros((TAIL, LANES), jnp.float32)
    for i, power in enumerate(powers):
        rows = power.shape[0]
        wide = jnp.broadcast_to(power, (rows, LANES)).astype(jnp.bfloat16)
        if rows < LANES:
            wide = jnp.concatenate([wide, jnp.zeros((LANES - rows, LANES), jnp.bfloat16)], axis=0)
        shape = (TAIL, LANES)
        pick = (lane_iota(shape, 0) == i) & (lane_iota(shape, 1) == 0)
        total = total + nt_dot(pick.astype(jnp.bfloat16), wide)
    return total.astype(jnp.int32).astype(jnp.int16)


def scale_of(tail, i, rows):
    held = tail.astype(jnp.int32).astype(jnp.float32)[i : i + 1, :]
    spread = jnp.broadcast_to(held, (LANES, LANES)).astype(jnp.bfloat16)
    shape = (LANES, LANES)
    unit = (lane_iota(shape, 0) == lane_iota(shape, 1)).astype(jnp.bfloat16)
    return (jnp.exp2(nt_dot(unit, spread)) * (1.0 / STEPS))[:rows]


def units_of(codes):
    return codes.astype(jnp.int32).astype(jnp.float32) + 32768.0


def prepare_kernel(leaf_count, mask_rows, mask_ref, label_ref, weight_ref, out_ref, onehot_ref):
    step = pl.program_id(0)
    rows, width = out_ref.shape
    share = width // leaf_count

    @pl.when(step == 0)
    def _():
        leaf = lax.axis_index("leaf")
        for d in range(leaf_count):
            start = pl.multiple_of(jnp.bitwise_xor(leaf, d) * share, share)
            wanted = label_ref[0, 0, :, pl.ds(start, share)]
            column = lane_iota((width, share), 0)
            onehot_ref[:, d * share : (d + 1) * share] = (column == wanted).astype(jnp.bfloat16)

    per = rows // mask_rows
    kept = []
    for i in range(per):
        part = weight_ref[0, 0, 0, i * mask_rows : (i + 1) * mask_rows, :]
        keep = mask_ref[0, 0, 0, step * per + i].astype(jnp.float32).astype(jnp.bfloat16)
        kept.append(part * keep)
    kept = jnp.concatenate(kept, axis=0)
    out_ref[...] = jnp.dot(
        kept, onehot_ref[...], preferred_element_type=jnp.float32
    ).astype(jnp.bfloat16)


def prepare(weights, mask, labels, leaf_count):
    feature, width = weights.shape[3:]
    mask_rows = feature // mask.shape[3]
    tile = min(feature, 4 * mask_rows)
    return pl.pallas_call(
        functools.partial(prepare_kernel, leaf_count, mask_rows),
        grid=(feature // tile,),
        in_specs=[
            SMEM,
            pl.BlockSpec((1, 1, 1, width), lambda i: (0, 0, 0, 0)),
            pl.BlockSpec((1, 1, 1, tile, width), lambda i: (0, 0, 0, i, 0)),
        ],
        out_specs=pl.BlockSpec((tile, width), lambda i: (i, 0)),
        out_shape=jax.ShapeDtypeStruct((feature, width), jnp.bfloat16),
        scratch_shapes=[pltpu.VMEM((width, width), jnp.bfloat16)],
        compiler_params=params(),
        cost_estimate=pl.CostEstimate(
            flops=2 * feature * width * width,
            bytes_accessed=4 * feature * width,
            transcendentals=0,
        ),
    )(mask, labels, weights)


def score_kernel(blocks, has_own, leaf_count, *refs):
    mine_refs, crossed_ref = refs[:blocks], refs[blocks]
    query_ref = refs[blocks + 1] if has_own else None
    weight_ref, own_ref, *sent_refs = refs[blocks + 1 + has_own :]
    level = lax.axis_index("level")
    levels = lax.axis_size("level")
    rows, half = mine_refs[0].shape
    share = own_ref.shape[1]
    near = pl.ds(pl.multiple_of(level * half, half), half)
    far = pl.ds(pl.multiple_of((levels - 1 - level) * half, half), half)
    mine = jnp.concatenate([ref[...] for ref in mine_refs], axis=0)
    other = crossed_ref[...]
    if has_own:
        other = jnp.concatenate([query_ref[:, far], other], axis=0)
    for d in range(leaf_count):
        columns = slice(d * share, (d + 1) * share)
        logits = jnp.dot(mine, weight_ref[near, columns], preferred_element_type=jnp.float32)
        logits = logits + jnp.dot(
            other, weight_ref[far, columns], preferred_element_type=jnp.float32
        )
        scores = jax.nn.sigmoid(logits)
        if d == 0:
            own_ref[...] = scores
        else:
            codes, power = encode(scores)
            out = sent_refs[d - 1]
            out[: blocks * rows, :] = codes
            out[blocks * rows :, :] = jnp.zeros((TAIL, share), jnp.int16)
            out[blocks * rows :, :LANES] = tail_of(
                [power[i * rows : (i + 1) * rows] for i in range(blocks)]
            )


def score(mine, crossed, queries, weights, leaf_count):
    blocks = len(mine)
    rows = mine[0].shape[0]
    feature, width = weights.shape
    share = width // leaf_count
    message = jax.ShapeDtypeStruct((blocks * rows + TAIL, share), jnp.int16)
    outs = [jax.ShapeDtypeStruct((blocks * rows, share), jnp.float32)] + [message] * (leaf_count - 1)
    operands = (*mine, crossed, *queries, weights)
    return pl.pallas_call(
        functools.partial(score_kernel, blocks, len(queries), leaf_count),
        in_specs=[VMEM] * len(operands),
        out_specs=[VMEM] * leaf_count,
        out_shape=outs,
        compiler_params=params(),
        cost_estimate=pl.CostEstimate(
            flops=2 * blocks * rows * feature * width,
            bytes_accessed=2 * feature * width,
            transcendentals=2 * blocks * rows * width,
        ),
    )(*operands)


def join_kernel(blocks, rows, *refs):
    own_ref = refs[0]
    got_refs = refs[1 : len(refs) - blocks]
    out_refs = refs[len(refs) - blocks :]
    share = own_ref.shape[1]
    powers = []
    for i in range(blocks):
        span = slice(i * rows, (i + 1) * rows)
        total = own_ref[span, :]
        for ref in got_refs:
            scale = scale_of(ref[blocks * rows :, :LANES], i, rows)
            scale = jnp.concatenate([scale] * (share // LANES), axis=1)
            total = total + units_of(ref[span, :]) * scale
        codes, power = encode(total)
        out_refs[i][:rows, :] = codes
        powers.append(power)
    tail = tail_of(powers)
    for ref in out_refs:
        ref[rows:, :] = jnp.zeros((TAIL, share), jnp.int16)
        ref[rows:, :LANES] = tail


def join(own, got, blocks):
    rows = own.shape[0] // blocks
    share = own.shape[1]
    message = jax.ShapeDtypeStruct((rows + TAIL, share), jnp.int16)
    return pl.pallas_call(
        functools.partial(join_kernel, blocks, rows),
        in_specs=[VMEM] * (1 + len(got)),
        out_specs=[VMEM] * blocks,
        out_shape=[message] * blocks,
        compiler_params=params(),
        cost_estimate=pl.CostEstimate(
            flops=40 * own.size, bytes_accessed=8 * own.size, transcendentals=0
        ),
    )(own, *got)


def collect_kernel(chunk, has_total, is_last, *refs):
    n = len(chunk)
    got, refs = refs[:n], refs[n:]
    before_ref, refs = (refs[0], refs[1:]) if has_total else (None, refs)
    beam_ref, refs = refs[0], refs[1:]
    if is_last:
        root_ref, parent_ref, out_ref, picked_ref = refs
    else:
        (out_ref,) = refs
    beam_len, rows, share = out_ref.shape
    me = lax.axis_index("group")
    beam = [jnp.broadcast_to(beam_ref[:, b : b + 1], (rows, LANES)) for b in range(beam_len)]
    gains, offsets = [], [0.0] * beam_len
    for i, k in enumerate(chunk):
        scale = scale_of(got[i][rows:, :LANES], i, rows)
        owner = jnp.bitwise_xor(me, k)
        gains.append([jnp.where(beam[b] == owner, scale, 0.0) for b in range(beam_len)])
        offsets = [offset + gain * 32768.0 for offset, gain in zip(offsets, gains[i])]
    if is_last:
        width = share * lax.axis_size("leaf")
        place = parent_ref[...]
        label = place % width - lax.axis_index("leaf") * share
        inside = (label >= 0) & (label < share)
        slot = place // width
        root = root_ref[...].astype(jnp.float32)
        target = jnp.where(inside, slot * share + label, -1)
        target = [jnp.broadcast_to(target[:, c : c + 1], (rows, LANES)) for c in range(beam_len)]
        picked = [jnp.zeros((rows, LANES), jnp.float32) for _ in range(beam_len)]
    for start in range(0, share, LANES):
        lanes = slice(start, start + LANES)
        totals = list(offsets)
        if has_total:
            totals = [totals[b] + before_ref[b, :, lanes] for b in range(beam_len)]
        for i in range(n):
            units = got[i][:rows, lanes].astype(jnp.int32).astype(jnp.float32)
            totals = [totals[b] + units * gains[i][b] for b in range(beam_len)]
        for b in range(beam_len):
            out_ref[b, :, lanes] = totals[b]
        if is_last:
            for b in range(beam_len):
                here = lane_iota((rows, LANES), 1) + (b * share + start)
                for c in range(beam_len):
                    picked[c] = picked[c] + jnp.where(here == target[c], totals[b], 0.0)
    if is_last:
        lane = lane_iota((rows, LANES), 1)
        out = jnp.zeros((rows, LANES), jnp.float32)
        for c in range(beam_len):
            parent = jnp.zeros((rows, 1), jnp.float32)
            for b in range(beam_len):
                parent = jnp.where(slot[:, c : c + 1] == b, root[:, b : b + 1], parent)
            out = jnp.where(lane == c, jnp.sum(picked[c], axis=1, keepdims=True) * parent, out)
        picked_ref[...] = out


def collect(chunk, got, before, beam, extra):
    rows, beam_len = beam.shape
    share = got[0].shape[1]
    operands = (*got, *before, beam, *extra)
    outs = [jax.ShapeDtypeStruct((beam_len, rows, share), jnp.float32)]
    if extra:
        outs.append(jax.ShapeDtypeStruct((rows, LANES), jnp.float32))
    return pl.pallas_call(
        functools.partial(collect_kernel, tuple(chunk), len(before), bool(extra)),
        in_specs=[VMEM] * len(operands),
        out_specs=[VMEM] * len(outs),
        out_shape=outs,
        compiler_params=params(),
        cost_estimate=pl.CostEstimate(
            flops=2 * len(got) * beam_len * rows * share,
            bytes_accessed=8 * beam_len * rows * share,
            transcendentals=0,
        ),
    )(*operands)


def finish_kernel(leaf_count, total_ref, root_ref, *refs):
    picked_refs, out_ref = refs[:leaf_count], refs[leaf_count]
    beam_len = total_ref.shape[0]
    second = picked_refs[0][...]
    for ref in picked_refs[1:]:
        second = second + ref[...]
    second = (second * (1.0 / leaf_count)).astype(jnp.bfloat16).astype(jnp.float32)[:, :beam_len]
    root = root_ref[...].astype(jnp.float32)
    parent = jnp.where(lax.axis_index("level") == 0, root, second)
    for b in range(beam_len):
        out_ref[:, b, :] = total_ref[b] * parent[:, b : b + 1]


def chunks_of(n):
    top = n // 2
    split = top + top // 2
    return [list(range(top, split)), list(range(split, n)), list(range(top))]


def low_bit(k):
    return k & -k


def body(queries, weights, block_mask, label_map, beam_lists, root_score, parent_pos):
    group_count = lax.axis_size("group")
    leaf_count = lax.axis_size("leaf")
    level_count = lax.axis_size("level")
    feature, label_width = weights.shape[3:]
    rows = queries.shape[0]
    beam_len = beam_lists.shape[2]
    share = label_width // leaf_count
    half = feature // level_count

    ordered = prepare(weights, block_mask, label_map, leaf_count)
    mine = {0: lax.dynamic_slice_in_dim(queries, lax.axis_index("level") * half, half, 1)}
    for k in range(1, group_count):
        low = low_bit(k)
        mine[k] = swapped(mine[k ^ low], "group", low)

    beam = beam_lists[0]
    chunks = chunks_of(group_count)
    total = []
    for i, chunk in enumerate(chunks):
        far = [k for k in chunk if k]
        joined = jnp.concatenate([mine[k] for k in far], axis=0)
        crossed = swapped(joined, "level", 1)
        own_queries = [] if len(far) == len(chunk) else [queries]
        own, *sent = score([mine[k] for k in chunk], crossed, own_queries, ordered, leaf_count)
        got = [swapped(message, "leaf", d) for d, message in enumerate(sent, 1)]
        back = [
            swapped(message, "group", k) if k else message
            for k, message in zip(chunk, join(own, got, len(chunk)))
        ]
        extra = (root_score, parent_pos) if i == len(chunks) - 1 else ()
        total = collect(chunk, back, total, beam, extra)
    total, picked = total

    handed = []
    for d in reversed(range(leaf_count)):
        route = [(leaf, leaf_count + (leaf ^ d)) for leaf in range(leaf_count)]
        handed.append(lax.ppermute(picked, ("level", "leaf"), route))
    scores = pl.pallas_call(
        functools.partial(finish_kernel, leaf_count),
        in_specs=[VMEM] * (2 + leaf_count),
        out_specs=VMEM,
        out_shape=jax.ShapeDtypeStruct((rows, beam_len, share), jnp.float32),
        compiler_params=params(),
    )(total, root_score, *handed)
    return scores[None]


def solution(mesh):
    in_specs = (
        P("group", None),
        P("level", "leaf", "group", None, None),
        P("level", "leaf", "group", None),
        P("level", "leaf", "group", None),
        P("level", "group", None),
        P("group", None),
        P("group", None),
    )
    out_specs = P("level", "group", None, "leaf")

    return jax.shard_map(body, mesh=mesh, in_specs=in_specs, out_specs=out_specs, check_vma=False)
```
